32 devices in a mesh: cfg: 2 (over y), ta: 4 (over z), xyz: 4 (over x, core).
Axes of the slice: x: 2, y: 2, z: 4, core: 2. Of those that a mesh axis runs over, the one named last changes fastest.
Arguments:
- sink: float32 [24, 4, 3, 2, 4, 32, 128], P('cfg', None, None, None, 'ta', 'xyz'), parts along dimension 0, may hold values from -6 to 6
- links: float32 [16, 4, 3, 3, 2, 4, 32, 128], P('cfg', None, None, None, None, 'ta', 'xyz'), parts along dimension 0, may hold values from -2 to 2
- section_index: int32 [2, 3], replicated, may hold values from 0 to 7
- momenta: int32 [33, 3], replicated, may hold values from -3 to 3
- source: int32 [3], replicated, may hold values from 0 to 15
Outputs:
- adjoint: float32 [24, 4, 3, 2, 4, 32, 128], P('cfg', None, None, None, 'ta', 'xyz'), parts along dimension 0
- correlator: float32 [4, 33, 4], P('cfg', None, 'ta'), parts along dimension 0
The draws below stay inside these ranges and needn't reach their ends.
There are 2 independent parts, one for each index of `cfg`. The reference program is written for one: setup_inputs(seed, part) draws one part's arguments, and reference() takes and returns one part's arrays. A program takes and returns all parts, laid end to end along the dimension named above; an argument that names none is the same for every part. Nothing has to cross between parts.
All inputs are finite; a program needn't handle non-finite values.
Results may differ from the reference program's by a relative error of at most 0.000068.
Values sent between devices are 32-bit elements; how exact they have to be, the bound alone decides.
A program may use at most 128 MiB of HBM per device.

```python
import math
import jax
import jax.numpy as jnp
from jax import lax

NCOL = 12
NMOM = 33
STEPS = 2
SLOTS = 8
LY = 16
NT = 4
NX = 32
NY = 16
NZ = 8


def touch_ends(drawn, rng, least, largest):
    dims = drawn.shape
    index_at = [jax.random.randint(jax.random.fold_in(rng, axis), (), 0, dims[axis]) for axis in range(len(dims))]
    drawn = drawn.at[tuple(index_at)].set(least)
    longest = dims.index(max(dims))
    index_at[longest] = (index_at[longest] + 1) % dims[longest]
    return drawn.at[tuple(index_at)].set(largest)


def block_scale(stream_key, shape, cuts, smallest, high):
    loudness = 1.0
    for position, blocks in cuts:
        draws = jax.random.uniform(jax.random.fold_in(jax.random.fold_in(stream_key, 6), position), (blocks,), jnp.float32, smallest / len(cuts), high / len(cuts))
        loudness = loudness * jnp.repeat(jnp.exp(draws), shape[position] // blocks).reshape((-1,) + (1,) * (len(shape) - 1 - position))
    return loudness


def bell_draw(rng, dims, spread, reach, pieces=(), held_as=jnp.bfloat16):
    result = jax.random.normal(rng, dims, jnp.float32) * spread
    if len(pieces) > 0:
        result = block_scale(rng, dims, pieces, -0.22, 0.18) * result
    return jnp.clip(result, min=-reach, max=reach).astype(held_as)


def setup_inputs(seed: int = 0, part: int = 0) -> dict:
    seeds = jax.random.split(jax.random.key(seed), 6)
    own_keys = jax.random.split(jax.random.fold_in(seeds[5], part), 6)
    return {
        "sink": bell_draw(own_keys[0], (NCOL, 4, 3, 2, NT, NX, NY * NZ), 1.0, 6.0, ((4, 4), (5, 4)), jnp.float32),
        "links": bell_draw(own_keys[1], (SLOTS, 4, 3, 3, 2, NT, NX, NY * NZ), 0.35, 2.0, ((5, 4), (6, 4)), jnp.float32),
        "section_index": touch_ends(jax.random.randint(seeds[2], (STEPS, 3), 0, SLOTS), jax.random.fold_in(seeds[2], 1), 0, SLOTS - 1).astype(jnp.int32),
        "momenta": touch_ends(jax.random.randint(seeds[3], (NMOM, 3), -3, 4), jax.random.fold_in(seeds[3], 1), -3, 3).astype(jnp.int32),
        "source": jax.random.randint(seeds[4], (3,), 0, LY).astype(jnp.int32),
    }


flow_step = 0.05

def hop_forward(matrix, field):
    spin_real = field[:, :, :, 0]
    spin_imag = field[:, :, :, 1]
    terms_real = []
    terms_imag = []
    for colour in range(3):
        link_real = matrix[:, colour, 0][None, None]
        link_imag = matrix[:, colour, 1][None, None]
        part_real = spin_real[:, :, colour][:, :, None]
        part_imag = spin_imag[:, :, colour][:, :, None]
        terms_real.append(link_real * part_real - link_imag * part_imag)
        terms_imag.append(link_real * part_imag + link_imag * part_real)
    return jnp.stack([terms_real[0] + terms_real[1] + terms_real[2], terms_imag[0] + terms_imag[1] + terms_imag[2]], axis=3)

def hop_backward(matrix, field):
    spin_real = field[:, :, :, 0]
    spin_imag = field[:, :, :, 1]
    terms_real = []
    terms_imag = []
    for colour in range(3):
        link_real = matrix[colour, :, 0][None, None]
        link_imag = matrix[colour, :, 1][None, None]
        part_real = spin_real[:, :, colour][:, :, None]
        part_imag = spin_imag[:, :, colour][:, :, None]
        terms_real.append(link_real * part_real + link_imag * part_imag)
        terms_imag.append(link_real * part_imag - link_imag * part_real)
    return jnp.stack([terms_real[0] + terms_real[1] + terms_real[2], terms_imag[0] + terms_imag[1] + terms_imag[2]], axis=3)

def shift_inner(field, amount):
    zcoord = jnp.arange(NY * NZ, dtype=jnp.int32) % NZ
    if amount < 0:
        inside = jnp.roll(field, -1, axis=-1)
        wrapped = jnp.roll(field, NZ - 1, axis=-1)
        return jnp.where(zcoord == NZ - 1, wrapped, inside)
    inside = jnp.roll(field, 1, axis=-1)
    wrapped = jnp.roll(field, 1 - NZ, axis=-1)
    return jnp.where(zcoord == 0, wrapped, inside)

def roll_lattice(field, direction, amount):
    if direction == 0:
        return jnp.roll(field, amount, axis=-3)
    if direction == 1:
        return jnp.roll(field, amount, axis=-2)
    if direction == 2:
        return jnp.roll(field, amount * NZ, axis=-1)
    return shift_inner(field, amount)

def laplacian(field, section_links):
    total = -8.0 * field
    for direction in range(4):
        matrix = section_links[direction]
        total = total + hop_forward(matrix, roll_lattice(field, direction, -1))
        total = total + roll_lattice(hop_backward(matrix, field), direction, 1)
    return total

def adjoint_step(lam, first, second, third):
    coef_third = 0.75 * flow_step
    coef_second = 8.0 * flow_step / 9.0
    coef_first = 0.25 * flow_step
    coef_mixed = 2.0 * flow_step / 9.0
    later = coef_third * laplacian(lam, third)
    middle = lam + coef_second * laplacian(later, second)
    return middle + later + laplacian(coef_first * middle - coef_mixed * later, first)

def phase_table(xcoord, nx_total, momenta, source):
    plane_index = jnp.arange(NY * NZ, dtype=jnp.int32)
    ycoord = plane_index // NZ
    zcoord = plane_index % NZ
    dist_x = jnp.mod(xcoord - source[0], nx_total)
    dist_y = jnp.mod(ycoord - source[1], NY)
    dist_z = jnp.mod(zcoord - source[2], NZ)
    frac_x = jnp.mod(momenta[:, 0:1] * dist_x[None, :], nx_total).astype(jnp.float32) / float(nx_total)
    frac_y = jnp.mod(momenta[:, 1:2] * dist_y[None, :], NY).astype(jnp.float32) / float(NY)
    frac_z = jnp.mod(momenta[:, 2:3] * dist_z[None, :], NZ).astype(jnp.float32) / float(NZ)
    frac = frac_x[:, :, None] + frac_y[:, None, :] + frac_z[:, None, :]
    angle = 2.0 * math.pi * frac
    table = jnp.concatenate([jnp.cos(angle), -jnp.sin(angle)], axis=0)
    return table.reshape(2 * NMOM, xcoord.shape[0] * NY * NZ)

def reference(sink, links, section_index, momenta, source):
    lam = sink
    for step in reversed(range(STEPS)):
        sections = [lax.dynamic_index_in_dim(links, section_index[step, section], 0, keepdims=False) for section in range(3)]
        lam = adjoint_step(lam, sections[0], sections[1], sections[2])
    squares = lax.optimization_barrier(jnp.sum(lam * lam, axis=(0, 2, 3)))
    density = squares[0] + squares[1] - squares[2] - squares[3]
    density = density.reshape(NT, NX * NY * NZ)
    table = phase_table(jnp.arange(NX, dtype=jnp.int32), NX, momenta, source)
    projected = jnp.dot(density, table.T, precision=lax.Precision.HIGHEST)
    scale = 1.0 / math.sqrt(576.0 * NX * NY * NZ)
    projected = projected * scale
    correlator = jnp.transpose(projected.reshape(NT, 2, NMOM), (1, 2, 0))
    return (lam, correlator)
```

```python
import functools
import math

import jax
import jax.numpy as jnp
from jax import lax
from jax.experimental import pallas as pl
from jax.experimental.pallas import tpu as pltpu
from jax.sharding import PartitionSpec as P

NMOM = 33
STEPS = 2
NY = 16
NZ = 8


flow_step = 0.05


def phase_table(xcoord, nx_total, momenta, source):
    plane_index = jnp.arange(NY * NZ, dtype=jnp.int32)
    ycoord = plane_index // NZ
    zcoord = plane_index % NZ
    dist_x = jnp.mod(xcoord - source[0], nx_total)
    dist_y = jnp.mod(ycoord - source[1], NY)
    dist_z = jnp.mod(zcoord - source[2], NZ)
    frac_x = jnp.mod(momenta[:, 0:1] * dist_x[None, :], nx_total).astype(jnp.float32) / float(
        nx_total
    )
    frac_y = jnp.mod(momenta[:, 1:2] * dist_y[None, :], NY).astype(jnp.float32) / float(NY)
    frac_z = jnp.mod(momenta[:, 2:3] * dist_z[None, :], NZ).astype(jnp.float32) / float(NZ)
    frac = frac_x[:, :, None] + frac_y[:, None, :] + frac_z[:, None, :]
    angle = 2.0 * math.pi * frac
    table = jnp.concatenate([jnp.cos(angle), -jnp.sin(angle)], axis=0)
    return table.reshape(2 * NMOM, xcoord.shape[0] * NY * NZ)


MESH = pl.DeviceIdType.MESH
SECTIONS = 3 * STEPS
BLOCK = 75


def remote(src, dst, send_sem, recv_sem, axis, peer):
    return pltpu.make_async_remote_copy(
        src_ref=src, dst_ref=dst, send_sem=send_sem, recv_sem=recv_sem,
        device_id={axis: peer}, device_id_type=MESH,
    )


def multiply(link, vec, conj):
    real = imag = None
    for k in range(3):
        if conj:
            lr, li = link[k, :, 0], link[k, :, 1]
        else:
            lr, li = link[:, k, 0], link[:, k, 1]
        vr, vi = vec[k, 0][None], vec[k, 1][None]
        if conj:
            r, i = lr * vr + li * vi, lr * vi - li * vr
        else:
            r, i = lr * vr - li * vi, lr * vi + li * vr
        real = r if real is None else real + r
        imag = i if imag is None else imag + i
    return real, imag


def roll3(x, amount, axis):
    shape = x.shape
    flat = x.reshape((-1,) + shape[-2:])
    return pltpu.roll(flat, amount % flat.shape[axis], axis).reshape(shape)


def kernel(n, nx, nc, sink_ref, link_ref, table_ref, out_ref, proj_ref,
           lam, later, mixed, lk, back, hs, hr, pj,
           loc_sem, fs_sem, fr_sem, us_sem, ur_sem, ds_sem, dr_sem,
           hss_sem, hsr_sem, os_sem, or_sem, ps_sem, pr_sem):
    me = lax.axis_index("ta")
    mx = lax.axis_index("xyz")
    left, right = lax.rem(mx + nx - 1, nx), lax.rem(mx + 1, nx)
    sub = lax.broadcasted_iota(jnp.int32, (8, 128), 0)
    zc = lax.broadcasted_iota(jnp.int32, (8, 128), 1) % NZ

    barrier = pltpu.get_barrier_semaphore()
    for d in range(1, n):
        pl.semaphore_signal(barrier, inc=1, device_id={"ta": lax.rem(me + d, n)}, device_id_type=MESH)
    for d in range(1, nx):
        pl.semaphore_signal(barrier, inc=1, device_id={"xyz": lax.rem(mx + d, nx)}, device_id_type=MESH)

    own = pltpu.make_async_copy(sink_ref.at[pl.ds(me * nc, nc)], lam.at[me], loc_sem.at[SECTIONS])
    own.start()
    for s in range(SECTIONS):
        pltpu.make_async_copy(link_ref.at[s], lk.at[s, me], loc_sem.at[s]).start()
    pl.semaphore_wait(barrier, n + nx - 2)

    def field_copy(d):
        peer = lax.rem(me + d, n)
        return remote(sink_ref.at[pl.ds(peer * nc, nc)], lam.at[me],
                      fs_sem.at[d - 1], fr_sem.at[d - 1], "ta", peer)

    for d in range(1, n):
        field_copy(d).start()

    def up_copy(s, h):
        blk = lax.rem(me - h + n, n)
        return remote(lk.at[s, blk], lk.at[s, blk], us_sem.at[s, h], ur_sem.at[s, h],
                      "ta", lax.rem(me + 1, n))

    def down_copy(s, h):
        blk = lax.rem(me + h, n)
        return remote(lk.at[s, blk], lk.at[s, blk], ds_sem.at[s, h], dr_sem.at[s, h],
                      "ta", lax.rem(me + n - 1, n))

    def has_up(h):
        return jnp.logical_and(me - h >= 0, me + 1 <= n - 1)

    def has_down(h):
        return jnp.logical_and(me + h <= n - 1, me - 1 >= 0)

    def start_hop(s, h):
        @pl.when(has_up(h))
        def _():
            up_copy(s, h).start()

        @pl.when(has_down(h))
        def _():
            down_copy(s, h).start()

    def wait_hop(s, h):
        @pl.when(me - 1 - h >= 0)
        def _():
            up_copy(s, h).wait_recv()

        @pl.when(me + 1 + h <= n - 1)
        def _():
            down_copy(s, h).wait_recv()

    for s in range(SECTIONS):
        pltpu.make_async_copy(link_ref.at[s], lk.at[s, me], loc_sem.at[s]).wait()
        if s < 2:
            start_hop(s, 0)
    own.wait()
    for d in range(1, n):
        field_copy(d).wait_recv()

    def halo_copy(s, side):
        peer = (left, right)[side]
        return remote(hs.at[s % 2, side], hr.at[s % 2, side], hss_sem.at[s, side],
                      hsr_sem.at[s, side], "xyz", peer)

    def put_halo(s, t, q, value):
        hs[s % 2, 0, t, q, 0:6] = value[:, 0, :]
        hs[s % 2, 1, t, q, 0:6] = value[:, 7, :]

    def first_halo(j, carry):
        t, q = j // nc, j % nc
        put_halo(0, t, q, lam[t, q])
        return carry

    lax.fori_loop(0, n * nc, first_halo, 0)
    for side in range(2):
        halo_copy(0, side).start()

    def lap(s, source, epilogue):
        par = s % 2

        def at_time(t, carry):
            prev, following = lax.rem(t + n - 1, n), lax.rem(t + 1, n)
            ux = lk[s, t, 18:36].reshape(18, 8, 128)
            ux = roll3(ux, 1, 1)
            for j in range(18):
                row = lk[s, t, 72 + j // 8, j % 8:j % 8 + 1, :]
                back[0, j] = jnp.where(sub == 0, jnp.broadcast_to(row, (8, 128)), ux[j])
            back[1] = roll3(lk[s, t, 36:54], NZ, 2)
            uz = lk[s, t, 54:72]
            back[2] = jnp.where((zc == 0)[None], roll3(uz, 1 - NZ, 2), roll3(uz, 1, 2))

            def links(ref_block):
                return ref_block.reshape(3, 3, 2, 8, 128)

            def at_spinor(q, inner):
                v = source[t, q]
                total_r = total_i = None

                def add(acc, r, i):
                    return (r, i) if acc is None else (acc[0] + r, acc[1] + i)

                def vec(x):
                    return x.reshape(3, 2, 8, 128)

                acc = None
                r, i = multiply(links(lk[s, t, 0:18]), vec(source[following, q]), False)
                acc = add(acc, r, i)
                r, i = multiply(links(lk[s, prev, 0:18]), vec(source[prev, q]), True)
                acc = add(acc, r, i)
                high = jnp.broadcast_to(hr[par, 0, t, q, 0:6][:, None, :], (6, 8, 128))
                low = jnp.broadcast_to(hr[par, 1, t, q, 0:6][:, None, :], (6, 8, 128))
                vf = jnp.where((sub == 7)[None], high, roll3(v, -1, 1))
                r, i = multiply(links(lk[s, t, 18:36]), vec(vf), False)
                acc = add(acc, r, i)
                vb = jnp.where((sub == 0)[None], low, roll3(v, 1, 1))
                r, i = multiply(links(back[0]), vec(vb), True)
                acc = add(acc, r, i)
                r, i = multiply(links(lk[s, t, 36:54]), vec(roll3(v, -NZ, 2)), False)
                acc = add(acc, r, i)
                r, i = multiply(links(back[1]), vec(roll3(v, NZ, 2)), True)
                acc = add(acc, r, i)
                vf = jnp.where((zc == NZ - 1)[None], roll3(v, NZ - 1, 2), roll3(v, -1, 2))
                r, i = multiply(links(lk[s, t, 54:72]), vec(vf), False)
                acc = add(acc, r, i)
                vb = jnp.where((zc == 0)[None], roll3(v, 1 - NZ, 2), roll3(v, 1, 2))
                r, i = multiply(links(back[2]), vec(vb), True)
                acc = add(acc, r, i)
                hop = jnp.stack([acc[0], acc[1]], axis=1).reshape(6, 8, 128)
                nxt = epilogue(t, q, hop - 8.0 * v, v)
                put_halo(s + 1, t, q, nxt)
                return inner

            lax.fori_loop(0, nc, at_spinor, 0)
            return carry

        lax.fori_loop(0, n, at_time, 0)

    def ep_later(t, q, value, v):
        value = (0.75 * flow_step) * value
        later[t, q] = value
        return value

    def ep_middle(t, q, value, v):
        middle = lam[t, q] + (8.0 * flow_step / 9.0) * value
        lam[t, q] = middle + v
        value = (0.25 * flow_step) * middle - (2.0 * flow_step / 9.0) * v
        mixed[t, q] = value
        return value

    def ep_last(t, q, value, v):
        value = lam[t, q] + value
        lam[t, q] = value
        return value

    def step_body(i, carry):
        for k, (source, epilogue) in enumerate(((lam, ep_later), (later, ep_middle), (mixed, ep_last))):
            s = i * 3 + k
            for h in range(n - 1):
                wait_hop(s, h)
                if h < n - 2:
                    start_hop(s, h + 1)

            @pl.when(s + 2 < SECTIONS)
            def _():
                start_hop(s + 2, 0)

            for side in range(2):
                halo_copy(s, side).wait()
            lap(s, source, epilogue)

            @pl.when(s + 1 < SECTIONS)
            def _():
                for side in range(2):
                    halo_copy(s + 1, side).start()
        return carry

    lax.fori_loop(0, STEPS, step_body, 0)

    def out_copy(d):
        peer = lax.rem(me + d, n)
        return remote(lam.at[peer], out_ref.at[pl.ds(me * nc, nc)],
                      os_sem.at[d - 1], or_sem.at[d - 1], "ta", peer)

    for d in range(1, n):
        out_copy(d).start()
    out_ref[pl.ds(me * nc, nc)] = lam[me]

    for d in range(1, n):
        field_copy(d).wait_send()

    def drain(s, carry):
        for h in range(n - 1):
            @pl.when(has_up(h))
            def _():
                up_copy(s, h).wait_send()

            @pl.when(has_down(h))
            def _():
                down_copy(s, h).wait_send()
        return carry

    lax.fori_loop(0, SECTIONS, drain, 0)
    for d in range(1, n):
        out_copy(d).wait()

    def squares(j, acc):
        block = out_ref[pl.ds(j * 4, 4)]
        sq = jnp.sum(block * block, axis=1)
        return acc + ((sq[0] + sq[1]) - (sq[2] + sq[3]))

    density = lax.fori_loop(0, sink_ref.shape[0] // 4, squares, jnp.zeros((8, 128), jnp.float32))
    pj[mx] = jnp.sum(table_ref[...] * density[None], axis=1)

    def proj_copy(d):
        return remote(pj.at[mx], pj.at[mx], ps_sem.at[d - 1], pr_sem.at[d - 1],
                      "xyz", lax.rem(mx + d, nx))

    for d in range(1, nx):
        proj_copy(d).start()
    for d in range(1, nx):
        proj_copy(d).wait()
    total = pj[0]
    for j in range(1, nx):
        total = total + pj[j]
    proj_ref[...] = jnp.broadcast_to(jnp.sum(total, axis=1, keepdims=True), total.shape)


def body(n, nx, sink, links, section_index, momenta, source):
    space_cells = sink.shape[5]
    spinors = sink.shape[0] * sink.shape[1]
    nc = spinors // n
    order = jnp.concatenate([section_index[step, ::-1] for step in reversed(range(STEPS))])
    chosen = jnp.take(links, order, axis=0).reshape(SECTIONS, 72, space_cells, NY * NZ)
    rows = chosen[:, 18:36, space_cells - 1, :]
    rows = lax.ppermute(rows, "xyz", [(i, (i + 1) % nx) for i in range(nx)])
    rows = jnp.pad(rows, ((0, 0), (0, 6), (0, 0))).reshape(SECTIONS, 3, 8, NY * NZ)
    blocks = jnp.concatenate([chosen, rows], axis=1)
    nx_total = space_cells * nx
    xcoord = lax.axis_index("xyz") * space_cells + jnp.arange(space_cells, dtype=jnp.int32)
    table = phase_table(xcoord, nx_total, momenta, source)
    table = table.reshape(2 * NMOM, space_cells, NY * NZ)
    tile = (space_cells, NY * NZ)
    field = pltpu.VMEM((n, nc, 6) + tile, jnp.float32)
    dma = pltpu.SemaphoreType.DMA
    out, proj = pl.pallas_call(
        functools.partial(kernel, n, nx, nc),
        out_shape=(
            jax.ShapeDtypeStruct((spinors, 6) + tile, jnp.float32),
            jax.ShapeDtypeStruct((2 * NMOM, NY * NZ), jnp.float32),
        ),
        in_specs=[
            pl.BlockSpec(memory_space=pl.ANY),
            pl.BlockSpec(memory_space=pl.ANY),
            pl.BlockSpec(memory_space=pltpu.VMEM),
        ],
        out_specs=(pl.BlockSpec(memory_space=pltpu.VMEM), pl.BlockSpec(memory_space=pltpu.VMEM)),
        scratch_shapes=[
            field, field, field,
            pltpu.VMEM((SECTIONS, n, BLOCK) + tile, jnp.float32),
            pltpu.VMEM((3, 18) + tile, jnp.float32),
            pltpu.VMEM((2, 2, n, nc, 8, NY * NZ), jnp.float32),
            pltpu.VMEM((2, 2, n, nc, 8, NY * NZ), jnp.float32),
            pltpu.VMEM((nx, 2 * NMOM, NY * NZ), jnp.float32),
            dma((SECTIONS + 1,)),
            dma((n - 1,)), dma((n - 1,)),
            dma((SECTIONS, n - 1)), dma((SECTIONS, n - 1)),
            dma((SECTIONS, n - 1)), dma((SECTIONS, n - 1)),
            dma((SECTIONS, 2)), dma((SECTIONS, 2)),
            dma((n - 1,)), dma((n - 1,)),
            dma((nx - 1,)), dma((nx - 1,)),
        ],
        compiler_params=pltpu.CompilerParams(
            collective_id=0, has_side_effects=True, vmem_limit_bytes=60 * 1024 * 1024
        ),
    )(sink.reshape((spinors, 6) + tile), blocks, table)
    scale = 1.0 / math.sqrt(576.0 * nx_total * NY * NZ)
    correlator = (proj[:, :1] * scale).reshape(2, NMOM, 1)
    return (out.reshape(sink.shape), correlator)


def solution(mesh):
    in_specs = (
        P("cfg", None, None, None, "ta", "xyz", None),
        P("cfg", None, None, None, None, "ta", "xyz", None),
        P(),
        P(),
        P(),
    )
    out_specs = (P("cfg", None, None, None, "ta", "xyz", None), P("cfg", None, "ta"))
    step = functools.partial(body, mesh.shape["ta"], mesh.shape["xyz"])
    return jax.shard_map(step, mesh=mesh, in_specs=in_specs, out_specs=out_specs, check_vma=False)
```

```python
import functools
import math

import jax
import jax.numpy as jnp
from jax import lax
from jax.experimental import pallas as pl
from jax.experimental.pallas import tpu as pltpu
from jax.sharding import PartitionSpec as P

NMOM = 33
STEPS = 2
NY = 16
NZ = 8


flow_step = 0.05


def phase_table(xcoord, nx_total, momenta, source):
    plane_index = jnp.arange(NY * NZ, dtype=jnp.int32)
    ycoord = plane_index // NZ
    zcoord = plane_index % NZ
    dist_x = jnp.mod(xcoord - source[0], nx_total)
    dist_y = jnp.mod(ycoord - source[1], NY)
    dist_z = jnp.mod(zcoord - source[2], NZ)
    frac_x = jnp.mod(momenta[:, 0:1] * dist_x[None, :], nx_total).astype(jnp.float32) / float(
        nx_total
    )
    frac_y = jnp.mod(momenta[:, 1:2] * dist_y[None, :], NY).astype(jnp.float32) / float(NY)
    frac_z = jnp.mod(momenta[:, 2:3] * dist_z[None, :], NZ).astype(jnp.float32) / float(NZ)
    frac = frac_x[:, :, None] + frac_y[:, None, :] + frac_z[:, None, :]
    angle = 2.0 * math.pi * frac
    table = jnp.concatenate([jnp.cos(angle), -jnp.sin(angle)], axis=0)
    return table.reshape(2 * NMOM, xcoord.shape[0] * NY * NZ)


MESH = pl.DeviceIdType.MESH
SECTIONS = 3 * STEPS
BLOCK = 75


def remote(src, dst, send_sem, recv_sem, axis, peer):
    return pltpu.make_async_remote_copy(
        src_ref=src, dst_ref=dst, send_sem=send_sem, recv_sem=recv_sem,
        device_id={axis: peer}, device_id_type=MESH,
    )


def multiply(link, vec, conj):
    real = imag = None
    for k in range(3):
        if conj:
            lr, li = link[k, :, 0], link[k, :, 1]
        else:
            lr, li = link[:, k, 0], link[:, k, 1]
        vr, vi = vec[k, 0][None], vec[k, 1][None]
        if conj:
            r, i = lr * vr + li * vi, lr * vi - li * vr
        else:
            r, i = lr * vr - li * vi, lr * vi + li * vr
        real = r if real is None else real + r
        imag = i if imag is None else imag + i
    return real, imag


def roll3(x, amount, axis):
    shape = x.shape
    flat = x.reshape((-1,) + shape[-2:])
    return pltpu.roll(flat, amount % flat.shape[axis], axis).reshape(shape)


def kernel(n, nx, nc, lo, hi, parts, sink_ref, link_ref, table_ref, out_ref, proj_ref,
           lam, later, mixed, lk, back, hs, hr, pj,
           loc_sem, fs_sem, fr_sem, us_sem, ur_sem, ds_sem, dr_sem,
           hss_sem, hsr_sem, os_sem, or_sem, ps_sem, pr_sem):
    me = lax.axis_index("ta")
    mx = lax.axis_index("xyz")
    worker = jnp.logical_and(me >= lo, me < hi)
    mine = me - lo
    share = nc // parts
    left, right = lax.rem(mx + nx - 1, nx), lax.rem(mx + 1, nx)
    sub = lax.broadcasted_iota(jnp.int32, (8, 128), 0)
    zc = lax.broadcasted_iota(jnp.int32, (8, 128), 1) % NZ

    barrier = pltpu.get_barrier_semaphore()
    for d in range(1, n):
        pl.semaphore_signal(barrier, inc=1, device_id={"ta": lax.rem(me + d, n)}, device_id_type=MESH)
    for d in range(1, nx):
        pl.semaphore_signal(barrier, inc=1, device_id={"xyz": lax.rem(mx + d, nx)}, device_id_type=MESH)

    def own_copy():
        return pltpu.make_async_copy(sink_ref.at[pl.ds(mine * nc, nc)], lam.at[me], loc_sem.at[SECTIONS])

    @pl.when(worker)
    def _():
        own_copy().start()

    for s in range(SECTIONS):
        pltpu.make_async_copy(link_ref.at[s], lk.at[s, me], loc_sem.at[s]).start()
    pl.semaphore_wait(barrier, n + nx - 2)

    def field_copy(j, source):
        return remote(sink_ref.at[pl.ds(j * nc, nc)], lam.at[source],
                      fs_sem.at[j], fr_sem.at[source], "ta", lo + j)

    for j in range(hi - lo):
        @pl.when(me != lo + j)
        def _():
            field_copy(j, me).start()

    def up_copy(s, h):
        blk = lax.rem(me - h + n, n)
        return remote(lk.at[s, blk], lk.at[s, blk], us_sem.at[s, h], ur_sem.at[s, h],
                      "ta", lax.rem(me + 1, n))

    def down_copy(s, h):
        blk = lax.rem(me + h, n)
        return remote(lk.at[s, blk], lk.at[s, blk], ds_sem.at[s, h], dr_sem.at[s, h],
                      "ta", lax.rem(me + n - 1, n))

    def has_up(h):
        return jnp.logical_and(me - h >= 0, me + 1 <= hi - 1)

    def has_down(h):
        return jnp.logical_and(me + h <= n - 1, me - 1 >= lo)

    def start_hop(s, h):
        @pl.when(has_up(h))
        def _():
            up_copy(s, h).start()

        @pl.when(has_down(h))
        def _():
            down_copy(s, h).start()

    def wait_hop(s, h):
        @pl.when(jnp.logical_and(me - 1 - h >= 0, me <= hi - 1))
        def _():
            up_copy(s, h).wait_recv()

        @pl.when(jnp.logical_and(me + 1 + h <= n - 1, me >= lo))
        def _():
            down_copy(s, h).wait_recv()

    for s in range(SECTIONS):
        pltpu.make_async_copy(link_ref.at[s], lk.at[s, me], loc_sem.at[s]).wait()
        if s < 2:
            start_hop(s, 0)
    @pl.when(worker)
    def _():
        own_copy().wait()
        for d in range(1, n):
            field_copy(0, lax.rem(me + d, n)).wait_recv()

    def halo_copy(s, side, part):
        peer = (left, right)[side]
        return remote(hs.at[s % 2, side, part], hr.at[s % 2, side, part], hss_sem.at[s, side, part],
                      hsr_sem.at[s, side, part], "xyz", peer)

    def put_halo(s, t, q, value):
        hs[s % 2, 0, q // share, t, q % share, 0:6] = value[:, 0, :]
        hs[s % 2, 1, q // share, t, q % share, 0:6] = value[:, 7, :]

    def first_halo(j, carry):
        t, q = j // nc, j % nc
        put_halo(0, t, q, lam[t, q])
        return carry

    @pl.when(worker)
    def _():
        lax.fori_loop(0, n * nc, first_halo, 0)
        for part in range(parts):
            for side in range(2):
                halo_copy(0, side, part).start()

    def prepare(s):
        def at_time(t, carry):
            ux = roll3(lk[s, t, 18:36], 1, 1)
            for j in range(18):
                row = lk[s, t, 72 + j // 8, j % 8:j % 8 + 1, :]
                back[t, 0, j] = jnp.where(sub == 0, jnp.broadcast_to(row, (8, 128)), ux[j])
            back[t, 1] = roll3(lk[s, t, 36:54], NZ, 2)
            uz = lk[s, t, 54:72]
            back[t, 2] = jnp.where((zc == 0)[None], roll3(uz, 1 - NZ, 2), roll3(uz, 1, 2))
            return carry

        lax.fori_loop(0, n, at_time, 0)

    def lap(s, part, source, epilogue):
        par = s % 2

        def at_time(t, carry):
            prev, following = lax.rem(t + n - 1, n), lax.rem(t + 1, n)

            def links(ref_block):
                return ref_block.reshape(3, 3, 2, 8, 128)

            def at_spinor(w, inner):
                q = part * share + w
                v = source[t, q]

                def add(acc, r, i):
                    return (r, i) if acc is None else (acc[0] + r, acc[1] + i)

                def vec(x):
                    return x.reshape(3, 2, 8, 128)

                acc = None
                r, i = multiply(links(lk[s, t, 0:18]), vec(source[following, q]), False)
                acc = add(acc, r, i)
                r, i = multiply(links(lk[s, prev, 0:18]), vec(source[prev, q]), True)
                acc = add(acc, r, i)
                high = jnp.broadcast_to(hr[par, 0, part, t, w, 0:6][:, None, :], (6, 8, 128))
                low = jnp.broadcast_to(hr[par, 1, part, t, w, 0:6][:, None, :], (6, 8, 128))
                vf = jnp.where((sub == 7)[None], high, roll3(v, -1, 1))
                r, i = multiply(links(lk[s, t, 18:36]), vec(vf), False)
                acc = add(acc, r, i)
                vb = jnp.where((sub == 0)[None], low, roll3(v, 1, 1))
                r, i = multiply(links(back[t, 0]), vec(vb), True)
                acc = add(acc, r, i)
                r, i = multiply(links(lk[s, t, 36:54]), vec(roll3(v, -NZ, 2)), False)
                acc = add(acc, r, i)
                r, i = multiply(links(back[t, 1]), vec(roll3(v, NZ, 2)), True)
                acc = add(acc, r, i)
                vf = jnp.where((zc == NZ - 1)[None], roll3(v, NZ - 1, 2), roll3(v, -1, 2))
                r, i = multiply(links(lk[s, t, 54:72]), vec(vf), False)
                acc = add(acc, r, i)
                vb = jnp.where((zc == 0)[None], roll3(v, 1 - NZ, 2), roll3(v, 1, 2))
                r, i = multiply(links(back[t, 2]), vec(vb), True)
                acc = add(acc, r, i)
                hop = jnp.stack([acc[0], acc[1]], axis=1).reshape(6, 8, 128)
                nxt = epilogue(t, q, hop - 8.0 * v, v)
                put_halo(s + 1, t, q, nxt)
                return inner

            lax.fori_loop(0, share, at_spinor, 0)
            return carry

        lax.fori_loop(0, n, at_time, 0)

    def ep_later(t, q, value, v):
        value = (0.75 * flow_step) * value
        later[t, q] = value
        return value

    def ep_middle(t, q, value, v):
        middle = lam[t, q] + (8.0 * flow_step / 9.0) * value
        lam[t, q] = middle + v
        value = (0.25 * flow_step) * middle - (2.0 * flow_step / 9.0) * v
        mixed[t, q] = value
        return value

    def ep_last(t, q, value, v):
        value = lam[t, q] + value
        lam[t, q] = value
        return value

    def out_copy(t, part, j):
        return remote(lam.at[t, pl.ds(part * share, share)],
                      out_ref.at[pl.ds(j * nc + part * share, share)],
                      os_sem.at[t, part], or_sem.at[j, part], "ta", t)

    hops = hi - 1

    def pass_on(s):
        for h in range(hops - 1):
            wait_hop(s, h)
            start_hop(s, h + 1)

    pass_on(0)

    def step_body(i, carry):
        for k, (source, epilogue) in enumerate(((lam, ep_later), (later, ep_middle), (mixed, ep_last))):
            s = i * 3 + k
            @pl.when(s + 1 < SECTIONS)
            def _():
                pass_on(s + 1)

            @pl.when(s + 2 < SECTIONS)
            def _():
                start_hop(s + 2, 0)

            wait_hop(s, hops - 1)

            @pl.when(worker)
            def _():
                prepare(s)

                def at_part(part, inner):
                    for side in range(2):
                        halo_copy(s, side, part).wait()
                    lap(s, part, source, epilogue)

                    @pl.when(s + 1 < SECTIONS)
                    def _():
                        for side in range(2):
                            halo_copy(s + 1, side, part).start()

                    @pl.when(s + 1 == SECTIONS)
                    def _():
                        for d in range(1, n):
                            out_copy(lax.rem(me + d, n), part, mine).start()
                    return inner

                lax.fori_loop(0, parts, at_part, 0)
        return carry

    lax.fori_loop(0, STEPS, step_body, 0)

    @pl.when(worker)
    def _():
        out_ref[pl.ds(mine * nc, nc)] = lam[me]

    for j in range(hi - lo):
        @pl.when(me != lo + j)
        def _():
            field_copy(j, me).wait_send()

    def drain(s, carry):
        for h in range(hops):
            @pl.when(has_up(h))
            def _():
                up_copy(s, h).wait_send()

            @pl.when(has_down(h))
            def _():
                down_copy(s, h).wait_send()
        return carry

    lax.fori_loop(0, SECTIONS, drain, 0)
    @pl.when(worker)
    def _():
        for part in range(parts):
            for d in range(1, n):
                out_copy(lax.rem(me + d, n), part, mine).wait_send()

    for j in range(hi - lo):
        @pl.when(me != lo + j)
        def _():
            for part in range(parts):
                out_copy(lo + j, part, j).wait_recv()

    def squares(j, acc):
        block = out_ref[pl.ds(j * 4, 4)]
        sq = jnp.sum(block * block, axis=1)
        return acc + ((sq[0] + sq[1]) - (sq[2] + sq[3]))

    density = lax.fori_loop(0, sink_ref.shape[0] // 4, squares, jnp.zeros((8, 128), jnp.float32))
    pj[mx] = jnp.sum(table_ref[...] * density[None], axis=1)

    def proj_copy(d):
        return remote(pj.at[mx], pj.at[mx], ps_sem.at[d - 1], pr_sem.at[d - 1],
                      "xyz", lax.rem(mx + d, nx))

    for d in range(1, nx):
        proj_copy(d).start()
    for d in range(1, nx):
        proj_copy(d).wait()
    total = pj[0]
    for j in range(1, nx):
        total = total + pj[j]
    proj_ref[...] = jnp.broadcast_to(jnp.sum(total, axis=1, keepdims=True), total.shape)


def body(n, nx, sink, links, section_index, momenta, source):
    space_cells = sink.shape[5]
    spinors = sink.shape[0] * sink.shape[1]
    lo = n // 4 if spinors % (n - 2 * (n // 4)) == 0 else 0
    hi = n - lo
    nc = spinors // (hi - lo)
    parts = 3 if nc % 3 == 0 else 1
    order = jnp.concatenate([section_index[step, ::-1] for step in reversed(range(STEPS))])
    chosen = jnp.take(links, order, axis=0).reshape(SECTIONS, 72, space_cells, NY * NZ)
    rows = chosen[:, 18:36, space_cells - 1, :]
    rows = lax.ppermute(rows, "xyz", [(i, (i + 1) % nx) for i in range(nx)])
    rows = jnp.pad(rows, ((0, 0), (0, 6), (0, 0))).reshape(SECTIONS, 3, 8, NY * NZ)
    blocks = jnp.concatenate([chosen, rows], axis=1)
    nx_total = space_cells * nx
    xcoord = lax.axis_index("xyz") * space_cells + jnp.arange(space_cells, dtype=jnp.int32)
    table = phase_table(xcoord, nx_total, momenta, source)
    table = table.reshape(2 * NMOM, space_cells, NY * NZ)
    tile = (space_cells, NY * NZ)
    field = pltpu.VMEM((n, nc, 6) + tile, jnp.float32)
    dma = pltpu.SemaphoreType.DMA
    out, proj = pl.pallas_call(
        functools.partial(kernel, n, nx, nc, lo, hi, parts),
        out_shape=(
            jax.ShapeDtypeStruct((spinors, 6) + tile, jnp.float32),
            jax.ShapeDtypeStruct((2 * NMOM, NY * NZ), jnp.float32),
        ),
        in_specs=[
            pl.BlockSpec(memory_space=pl.ANY),
            pl.BlockSpec(memory_space=pl.ANY),
            pl.BlockSpec(memory_space=pltpu.VMEM),
        ],
        out_specs=(pl.BlockSpec(memory_space=pltpu.VMEM), pl.BlockSpec(memory_space=pltpu.VMEM)),
        scratch_shapes=[
            field, field, field,
            pltpu.VMEM((SECTIONS, n, BLOCK) + tile, jnp.float32),
            pltpu.VMEM((n, 3, 18) + tile, jnp.float32),
            pltpu.VMEM((2, 2, parts, n, nc // parts, 8, NY * NZ), jnp.float32),
            pltpu.VMEM((2, 2, parts, n, nc // parts, 8, NY * NZ), jnp.float32),
            pltpu.VMEM((nx, 2 * NMOM, NY * NZ), jnp.float32),
            dma((SECTIONS + 1,)),
            dma((hi - lo,)), dma((n,)),
            dma((SECTIONS, n - 1)), dma((SECTIONS, n - 1)),
            dma((SECTIONS, n - 1)), dma((SECTIONS, n - 1)),
            dma((SECTIONS, 2, parts)), dma((SECTIONS, 2, parts)),
            dma((n, parts)), dma((hi - lo, parts)),
            dma((nx - 1,)), dma((nx - 1,)),
        ],
        compiler_params=pltpu.CompilerParams(
            collective_id=0, has_side_effects=True, vmem_limit_bytes=60 * 1024 * 1024
        ),
    )(sink.reshape((spinors, 6) + tile), blocks, table)
    scale = 1.0 / math.sqrt(576.0 * nx_total * NY * NZ)
    correlator = (proj[:, :1] * scale).reshape(2, NMOM, 1)
    return (out.reshape(sink.shape), correlator)


def solution(mesh):
    in_specs = (
        P("cfg", None, None, None, "ta", "xyz", None),
        P("cfg", None, None, None, None, "ta", "xyz", None),
        P(),
        P(),
        P(),
    )
    out_specs = (P("cfg", None, None, None, "ta", "xyz", None), P("cfg", None, "ta"))
    step = functools.partial(body, mesh.shape["ta"], mesh.shape["xyz"])
    return jax.shard_map(step, mesh=mesh, in_specs=in_specs, out_specs=out_specs, check_vma=False)
```
